32 devices in a mesh: gx: 4 (over x, core), gy: 4 (over z), gz: 2 (over y).
Axes of the slice: x: 2, y: 2, z: 4, core: 2. Of those that a mesh axis runs over, the one named last changes fastest.
Arguments:
- particles: float32 [4096, 512], P(('gx', 'gy', 'gz')), may hold values from -6 to 6
- scores: bfloat16 [4096, 512], P(('gx', 'gy', 'gz')), may hold values from -6 to 6
- band_power: int32 [512], replicated, may hold values from 7 to 8
Outputs:
- drift: float32 [4096, 512], P(('gx', 'gy', 'gz'))
The draws below stay inside these ranges and needn't reach their ends.
All inputs are finite; a program needn't handle non-finite values.
Results may differ from the reference program's by a relative error of at most 0.0046.
Values may be sent and summed in bfloat16 or wider, within the bound.
No kernel may reach another device: no remote copies, remote signals or barrier semaphores. Data moves between devices by JAX's collectives and lax.ppermute only.
A program may use at most 64 MiB of HBM per device.

```python
import jax
import jax.numpy as jnp
from jax import lax

D = 512
PARTICLES = 4096


latent_dims = 16


def draw_particles(key, part):
    keys = jax.random.split(jax.random.fold_in(key, 11), 3)
    latent_scale = 0.75 ** 0.5
    basis = jax.random.normal(keys[0], (latent_dims, D), jnp.float32) / latent_dims ** 0.5
    coords = jax.random.normal(keys[1], (PARTICLES, latent_dims), jnp.float32) * latent_scale
    noise = jax.random.normal(keys[2], (PARTICLES, D), jnp.float32) * 0.5
    values = jnp.dot(coords, basis, precision=lax.Precision.HIGHEST) + noise
    return jnp.clip(values, -6.0, 6.0)


def with_ends(drawn, own_key, smallest, largest):
    shape = drawn.shape
    index_at = [jax.random.randint(jax.random.fold_in(own_key, axis), (), 0, shape[axis]) for axis in range(len(shape))]
    drawn = drawn.at[tuple(index_at)].set(smallest)
    longest = shape.index(max(shape))
    index_at[longest] = (index_at[longest] + 1) % shape[longest]
    return drawn.at[tuple(index_at)].set(largest)


def level_of(stream_key, dims, cuts, least, largest):
    loudness = 1.0
    for dim, parts in cuts:
        draws = jax.random.uniform(jax.random.fold_in(jax.random.fold_in(stream_key, 6), dim), (parts,), jnp.float32, least / len(cuts), largest / len(cuts))
        loudness = loudness * jnp.repeat(jnp.exp(draws), dims[dim] // parts).reshape((-1,) + (1,) * (len(dims) - 1 - dim))
    return loudness


def gaussian(stream_key, extent, scale, limit, shards=(), dtype=jnp.bfloat16):
    values = scale * jax.random.normal(stream_key, extent, jnp.float32)
    if shards:
        values = values * level_of(stream_key, extent, shards, -0.22, 0.18)
    return jnp.clip(values, -limit, limit).astype(dtype)


def setup_inputs(seed: int = 0) -> dict:
    key_of = jax.random.split(jax.random.key(seed), 4)
    return {
        "particles": draw_particles(jax.random.fold_in(key_of[3], 71), 0),
        "scores": gaussian(key_of[1], (PARTICLES, D), 1.0, 6.0, ((0, 32),)),
        "band_power": with_ends(jax.random.randint(key_of[2], (D,), 7, 9), jax.random.fold_in(key_of[2], 1), 7, 8).astype(jnp.int32),
    }


def kernel_terms(target_rows, sources, stacked, source_squares, weights):
    target_float = target_rows.astype(jnp.float32)
    target_squares = jnp.sum(jnp.square(target_float) * weights[None, :], axis=1)
    scaled = (target_float * weights[None, :]).astype(jnp.bfloat16)
    inner = lax.dot_general(scaled, sources, (((1,), (1,)), ((), ())), preferred_element_type=jnp.float32)
    distance = target_squares[:, None] + source_squares[None, :] - 2.0 * inner
    kernel = jnp.exp(-distance).astype(jnp.bfloat16)
    products = jnp.dot(kernel, stacked, preferred_element_type=jnp.float32)
    totals = jnp.sum(kernel.astype(jnp.float32), axis=1)
    width = target_rows.shape[1]
    return products[:, :width] + 2.0 * weights[None, :] * (target_float * totals[:, None] - products[:, width:])


def reference(particles, scores, band_power):
    weights = jnp.exp2(-band_power.astype(jnp.float32))
    rounded = particles.astype(jnp.bfloat16)
    source_squares = jnp.sum(jnp.square(rounded.astype(jnp.float32)) * weights[None, :], axis=1)
    stacked = jnp.concatenate([scores, rounded], axis=1)
    total_rows = rounded.shape[0]
    block_rows = 512 if total_rows % 512 == 0 else total_rows
    target_blocks = rounded.reshape(total_rows // block_rows, block_rows, rounded.shape[1])

    def one_block(target_rows):
        return kernel_terms(target_rows, rounded, stacked, source_squares, weights)

    drift = lax.map(one_block, target_blocks)
    return drift.reshape(total_rows, rounded.shape[1])
```

```python
import jax
import jax.numpy as jnp
from jax import lax
from jax.experimental import pallas as pl
from jax.experimental.pallas import tpu as pltpu
from jax.sharding import PartitionSpec as P

AXES = ("gx", "gy", "gz")


def partner(index, step, size):
    return index ^ step if size & (size - 1) == 0 else (index + step) % size


def along_gy(value, step, size, back=False):
    pairs = [(i, partner(i, step, size)) for i in range(size)]
    return lax.ppermute(value, "gy", [(b, a) for a, b in pairs] if back else pairs)


def along_plane(value, step_gx, step_gz, size_gx, size_gz):
    chips = size_gx // 2
    pairs = []
    for gx in range(size_gx):
        for gz in range(size_gz):
            to_gx = partner(gx // 2, step_gx, chips) * 2 + gx % 2
            pairs.append((gx * size_gz + gz, to_gx * size_gz + partner(gz, step_gz, size_gz)))
    return lax.ppermute(value, ("gx", "gz"), pairs)


def to_sibling(value, size_gx):
    return lax.ppermute(value, "gx", [(i, i ^ 1) for i in range(size_gx)])


def terms(targets, source_rows, source_scores, band_row, out_dtypes):
    n_targets, n_sources = len(targets), len(source_rows)
    rows, width = targets[0].shape

    def body(*refs):
        band_ref = refs[0]
        target_refs = refs[1 : 1 + n_targets]
        row_refs = refs[1 + n_targets : 1 + n_targets + n_sources]
        score_refs = refs[1 + n_targets + n_sources : 1 + n_targets + 2 * n_sources]
        out_refs = refs[1 + n_targets + 2 * n_sources :]
        weights = jnp.exp2(-band_ref[...].astype(jnp.float32))
        target_float = jnp.concatenate([r[...] for r in target_refs], axis=0).astype(jnp.float32)
        scaled_float = target_float * weights
        target_squares = jnp.sum(target_float * scaled_float, axis=1, keepdims=True)
        scaled = scaled_float.astype(jnp.bfloat16)
        ones = jnp.ones((8, width), jnp.bfloat16)
        over_lanes = (((1,), (1,)), ((), ()))
        kernels = []
        for ref in row_refs:
            source = ref[...]
            source_float = source.astype(jnp.float32)
            square = source_float * source_float * weights
            high = square.astype(jnp.bfloat16)
            low = (square - high.astype(jnp.float32)).astype(jnp.bfloat16)
            source_squares = lax.dot_general(
                ones, high, over_lanes, preferred_element_type=jnp.float32
            ) + lax.dot_general(ones, low, over_lanes, preferred_element_type=jnp.float32)
            inner = lax.dot_general(scaled, source, over_lanes, preferred_element_type=jnp.float32)
            distance = target_squares + source_squares[0:1, :] - 2.0 * inner
            kernels.append(jnp.exp(-distance).astype(jnp.bfloat16))
        kernel = jnp.concatenate(kernels, axis=1)
        totals = jnp.sum(kernel.astype(jnp.float32), axis=1, keepdims=True)
        attract = jnp.dot(
            kernel, jnp.concatenate([r[...] for r in score_refs], axis=0), preferred_element_type=jnp.float32
        )
        center = jnp.dot(
            kernel, jnp.concatenate([r[...] for r in row_refs], axis=0), preferred_element_type=jnp.float32
        )
        drift = attract + 2.0 * weights * (target_float * totals - center)
        for i, ref in enumerate(out_refs):
            ref[...] = drift[i * rows : (i + 1) * rows].astype(ref.dtype)

    whole = pl.BlockSpec(memory_space=pltpu.VMEM)
    return pl.pallas_call(
        body,
        out_shape=[jax.ShapeDtypeStruct((rows, width), d) for d in out_dtypes],
        in_specs=[whole] * (1 + n_targets + 2 * n_sources),
        out_specs=[whole] * len(out_dtypes),
        compiler_params=pltpu.CompilerParams(vmem_limit_bytes=60 * 1024 * 1024),
    )(band_row, *targets, *source_rows, *source_scores)


def make_local(shape):
    size_gx, size_gy, size_gz = shape["gx"], shape["gy"], shape["gz"]

    def local(particles, scores, band_power):
        band_row = band_power[None, :]
        rounded = particles.astype(jnp.bfloat16)
        steps = sorted(range(1, size_gy), key=lambda k: -min(k, size_gy - k))
        far = {k: along_gy(rounded, k, size_gy) for k in steps}
        plane = [(a, b) for a in range(size_gx // 2) for b in range(size_gz) if a or b]
        rows, scs = [rounded], [scores]
        for a, b in plane:
            rows.append(along_plane(rounded, a, b, size_gx, size_gz))
            scs.append(along_plane(scores, a, b, size_gx, size_gz))
        rows += [to_sibling(r, size_gx) for r in rows]
        scs += [to_sibling(r, size_gx) for r in scs]
        half = len(steps) - len(steps) // 2
        first, second = steps[:half], steps[half:]
        bf16 = jnp.bfloat16
        out_first = terms([far[k] for k in first], rows, scs, band_row, [bf16] * len(first))
        back = {k: along_gy(o, k, size_gy, back=True) for k, o in zip(first, out_first)}
        out_second = terms(
            [far[k] for k in second] + [rounded], rows, scs, band_row, [bf16] * len(second) + [jnp.float32]
        )
        back.update({k: along_gy(o, k, size_gy, back=True) for k, o in zip(second, out_second)})
        drift = out_second[-1]
        for k in steps:
            drift = drift + back[k].astype(jnp.float32)
        return drift

    return local


def solution(mesh):
    spec = P(AXES, None)
    return jax.shard_map(
        make_local(dict(mesh.shape)), mesh=mesh, in_specs=(spec, spec, P()), out_specs=spec, check_vma=False
    )
```
